32 devices in a mesh: dom: 8 (over z, y), sub: 4 (over x, core).
Axes of the slice: x: 2, y: 2, z: 4, core: 2. Of those that a mesh axis runs over, the one named last changes fastest.
Arguments:
- positions: float32 [2048, 3, 256], P(('dom', 'sub')), may hold values from -6 to 6
- time_bins: int32 [2048, 256], P(('dom', 'sub')), may hold values from 0 to 5
- home_groups: int32 [2048], P(('dom', 'sub')), may hold values from 0 to 63
- targets: int32 [2048, 4], P(('dom', 'sub')), may hold values from -1 to 7, as said below
- target_groups: int32 [2048, 4], P(('dom', 'sub')), may hold values from 0 to 63
- node_pos: float32 [3, 131072], P(None, ('dom', 'sub')), may hold values from -6 to 6
- node_mass: float32 [131072], P(('dom', 'sub')), may hold values from 0.2 to 2
- node_lists: int32 [512, 256], P('dom'), may hold values from 0 to 16383
- list_counts: int32 [512], P('dom'), may hold values from 64 to 256, as said below
Outputs:
- forces: float32 [2048, 3, 256], P(('dom', 'sub'))
The draws below stay inside these ranges and needn't reach their ends.
Inputs may be any that keep to these rules, and one draw needn't show every extreme that they name: `targets`: row b names the remote domains that block b visits, each at most once and never its own domain b // 256; -1 marks an unused entry, in any column. The rows of one device name one domain at most 32 times, and some device names some domain exactly 32 times in every draw. The rows of one domain's 4 devices together name one domain at most 64 times, and this is reached in every draw. `list_counts`: each domain has at least one list with all 256 entries valid.
All inputs are finite; a program needn't handle non-finite values.
Results may differ from the reference program's by a relative error of at most 0.0003.
Values sent between devices are 32-bit elements; how exact they have to be, the bound alone decides.
A program may use at most 128 MiB of HBM per device.

```python
import math
import jax
import jax.numpy as jnp
from jax import lax

BLOCK = 256
BLK_DEV = 64
TOP = 4
LIST = 256
GROUPS = 64
NODE_DEV = 4096
BINS = 6
CUR_BIN = 2
BLOCKS = 2048
NODES = 131072
CAP = 32
CAP_ROW = 64
N_DOM = 8
N_SUB = 4


def draw_list_counts(key, part):
    count_key = jax.random.fold_in(key, 11)
    full_key = jax.random.fold_in(key, 12)
    counts = jax.random.randint(count_key, (N_DOM, GROUPS), LIST // 4, LIST + 1)
    full_list = jax.random.randint(full_key, (N_DOM,), 0, GROUPS)
    counts = jnp.where(jnp.arange(GROUPS)[None, :] == full_list[:, None], LIST, counts)
    return counts.reshape(N_DOM * GROUPS).astype(jnp.int32)


def draw_targets(key, part):
    hot_key = jax.random.fold_in(key, 21)
    order_key = jax.random.fold_in(key, 22)
    level_key = jax.random.fold_in(key, 23)
    wish_key = jax.random.fold_in(key, 24)
    block_key = jax.random.fold_in(key, 25)
    column_key = jax.random.fold_in(key, 26)
    hot_domain = jax.random.randint(hot_key, (), 0, N_DOM)
    domain_ids = jnp.arange(N_DOM, dtype=jnp.int32)
    orders = jax.vmap(lambda one_key: jax.random.permutation(one_key, N_SUB))(jax.random.split(order_key, N_DOM))
    levels = jax.random.randint(level_key, (N_DOM, N_SUB, 1), 0, 4)
    wishes = jnp.minimum(CAP, jax.random.randint(wish_key, (N_DOM, N_SUB, N_DOM), 0, CAP + 1) * levels // 2)
    wishes = jnp.where(domain_ids[None, None, :] == hot_domain, CAP, wishes)
    wishes = jnp.where(domain_ids[:, None, None] == domain_ids[None, None, :], 0, wishes).astype(jnp.int32)
    rotation = (hot_domain + domain_ids) % N_DOM
    unrotate = (domain_ids - hot_domain) % N_DOM
    budget = BLK_DEV * TOP

    def row_counts(row_wishes, row_order):

        def advance(already, position):
            wanted = jnp.minimum(row_wishes[row_order[position]], CAP_ROW - already)
            turned = wanted[rotation]
            before = jnp.cumsum(turned) - turned
            granted = jnp.maximum(jnp.minimum(turned, budget - before), 0)[unrotate]
            return (already + granted, granted)
        _, granted = lax.scan(advance, jnp.zeros((N_DOM,), jnp.int32), jnp.arange(N_SUB))
        return jnp.zeros((N_SUB, N_DOM), jnp.int32).at[row_order].set(granted)
    counts = jax.vmap(row_counts)(wishes, orders).reshape(N_DOM * N_SUB, N_DOM)
    tickets = jnp.arange(budget, dtype=jnp.int32)

    def device_table(device_counts, shuffle_key, order_keys):
        boundaries = jnp.cumsum(device_counts)
        ticket_domain = jnp.sum((boundaries[None, :] <= tickets[:, None]).astype(jnp.int32), axis=1)
        ticket_domain = jnp.where(tickets < boundaries[-1], ticket_domain, -1)
        assigned = ticket_domain.reshape(TOP, BLK_DEV).T
        assigned = assigned[jax.random.permutation(shuffle_key, BLK_DEV)]
        column_orders = jax.vmap(lambda one_key: jax.random.permutation(one_key, TOP))(jax.random.split(order_keys, BLK_DEV))
        return jnp.take_along_axis(assigned, column_orders, axis=1)
    device_total = N_DOM * N_SUB
    tables = jax.vmap(device_table)(counts, jax.random.split(block_key, device_total), jax.random.split(column_key, device_total))
    return tables.reshape(device_total * BLK_DEV, TOP).astype(jnp.int32)


def set_ends(array, own_key, smallest, largest):
    dims = array.shape
    index_at = [jax.random.randint(jax.random.fold_in(own_key, axis), (), 0, dims[axis]) for axis in range(len(dims))]
    array = array.at[tuple(index_at)].set(smallest)
    longest = dims.index(max(dims))
    index_at[longest] = (index_at[longest] + 1) % dims[longest]
    return array.at[tuple(index_at)].set(largest)


def shard_levels(stream_key, shape, cuts, smallest, largest):
    factor_of, own = 1.0, jax.random.fold_in(stream_key, 6)
    for axis_at, blocks in cuts:
        draws = jnp.exp(jax.random.uniform(jax.random.fold_in(own, axis_at), (blocks,), jnp.float32, smallest / len(cuts), largest / len(cuts)))
        factor_of = factor_of * jnp.repeat(draws, shape[axis_at] // blocks).reshape([-1 if axis == axis_at else 1 for axis in range(len(shape))])
    return factor_of


def bell_draw(key, extent, scale, most, pieces=(), kind=jnp.bfloat16):
    values = jax.random.normal(key, extent, jnp.float32) * scale
    if len(pieces) > 0:
        values = shard_levels(key, extent, pieces, -0.22, 0.18) * values
    return jnp.clip(values, min=-most, max=most).astype(kind)


def setup_inputs(seed: int = 0) -> dict:
    seeds = jax.random.split(jax.random.key(seed), 10)
    positions = bell_draw(seeds[0], (BLOCKS, 3, BLOCK), 1.0, 6.0, ((0, 32),), jnp.float32)
    time_bins = set_ends(jax.random.randint(seeds[1], (BLOCKS, BLOCK), 0, BINS), jax.random.fold_in(seeds[1], 1), 0, BINS - 1).astype(jnp.int32)
    home_groups = set_ends(jax.random.randint(seeds[2], (BLOCKS,), 0, GROUPS), jax.random.fold_in(seeds[2], 1), 0, GROUPS - 1).astype(jnp.int32)
    targets = draw_targets(jax.random.fold_in(seeds[9], 71), 0)
    target_groups = set_ends(jax.random.randint(seeds[4], (BLOCKS, TOP), 0, GROUPS), jax.random.fold_in(seeds[4], 1), 0, GROUPS - 1).astype(jnp.int32)
    node_pos = bell_draw(seeds[5], (3, NODES), 1.0, 6.0, ((1, 32),), jnp.float32)
    node_mass = jnp.clip(jnp.exp(math.log(2.0) - 2.3025851 * jax.random.uniform(seeds[6], (NODES,), jnp.float32) ** shard_levels(seeds[6], (NODES,), ((0, 32),), -0.2, 0.2)), 0.2, 2.0)
    node_lists = set_ends(jax.random.randint(seeds[7], (N_DOM * GROUPS, LIST), 0, NODE_DEV * N_SUB), jax.random.fold_in(seeds[7], 1), 0, (NODE_DEV * N_SUB) - 1).astype(jnp.int32)
    list_counts = draw_list_counts(jax.random.fold_in(seeds[9], 71), 0)
    return dict(positions=positions, time_bins=time_bins, home_groups=home_groups, targets=targets, target_groups=target_groups, node_pos=node_pos, node_mass=node_mass, node_lists=node_lists, list_counts=list_counts)


soften_sq = 0.04
gauss_slope = 1.1283791670955126

def short_pull(sink_pos, source_pos, source_mass):
    offset = sink_pos[:, None, :] - source_pos[:, :, None]
    range_sq = lax.optimization_barrier(jnp.sum(offset * offset, axis=0)) + soften_sq
    distance = jnp.sqrt(range_sq)
    scaled = distance * 0.5
    factor = lax.erfc(scaled) + gauss_slope * scaled * jnp.exp(-scaled * scaled)
    weight = source_mass[:, None] * factor / (range_sq * distance)
    return -lax.optimization_barrier(jnp.sum(offset * weight[None, :, :], axis=1))

def reference(positions, time_bins, home_groups, targets, target_groups, node_pos, node_mass, node_lists, list_counts):
    per_domain = BLK_DEV * N_SUB
    node_count = NODE_DEV * N_SUB
    block_ids = jnp.arange(BLOCKS, dtype=jnp.int32)
    home_domain = block_ids // per_domain
    visit_domain = jnp.concatenate([home_domain[:, None], jnp.maximum(targets, 0)], axis=1).astype(jnp.int32)
    visit_group = jnp.concatenate([home_groups[:, None], target_groups], axis=1).astype(jnp.int32)
    visit_alive = jnp.concatenate([jnp.ones((BLOCKS, 1), jnp.float32), (targets >= 0).astype(jnp.float32)], axis=1)
    list_rows = visit_domain * GROUPS + visit_group
    entry_ids = jnp.arange(LIST, dtype=jnp.int32)

    def one_visit(sink_pos, list_row, domain_id, is_alive):
        node_index = node_lists[list_row] + domain_id * node_count
        node_weight = node_mass[node_index] * (entry_ids < list_counts[list_row]).astype(jnp.float32) * is_alive
        return short_pull(sink_pos, node_pos[:, node_index], node_weight)

    def one_block(sink_pos, block_rows, block_domains, block_alive):
        pulls = jax.vmap(one_visit, in_axes=(None, 0, 0, 0))(sink_pos, block_rows, block_domains, block_alive)
        return lax.optimization_barrier(jnp.sum(pulls, axis=0))

    def one_group(operands):
        return jax.vmap(one_block)(*operands)
    grouped = lax.map(one_group, (positions.reshape(BLOCKS // 8, 8, 3, BLOCK), list_rows.reshape(BLOCKS // 8, 8, TOP + 1), visit_domain.reshape(BLOCKS // 8, 8, TOP + 1), visit_alive.reshape(BLOCKS // 8, 8, TOP + 1)))
    summed = grouped.reshape(BLOCKS, 3, BLOCK)
    active = (time_bins <= CUR_BIN).astype(jnp.float32)
    return summed * active[:, None, :]
```

```python
import functools
import math

import jax
import jax.numpy as jnp
from jax import lax
from jax.experimental import pallas as pl
from jax.experimental.pallas import tpu as pltpu
from jax.sharding import PartitionSpec as P

CUR_BIN = 2
SOFTEN_SQ = 0.04
LANES = 128
SCALE = math.sqrt(math.log2(math.e) / 4)
SLOPE = 1.0 / (math.sqrt(math.pi) * SCALE)
SHIFT = 3.303086624162737
POLY = (
    0.7187441716120562,
    2.51274456019257,
    4.689033408702265,
    49.73417752543693,
    -125.5838890131009,
    722.0978767862518,
    -720.5249114117939,
)
STEP = 72


def gather_kernel(nodes, ids, counts, out):
    sharers, _, table_rows, _ = nodes.shape
    rows = ids.shape[0]
    index = ids[...]
    high = index >> 7
    low = index & (LANES - 1)
    for owner in range(sharers):

        def one(step, found):
            for sub_step in range(2):
                row = step * 2 + sub_step
                here = high == owner * table_rows + row
                fresh = []
                for feature in range(4):
                    line = jnp.broadcast_to(nodes[owner, feature, pl.ds(row, 1), :], (rows, LANES))
                    value = jnp.take_along_axis(line, low, axis=1, mode="promise_in_bounds")
                    fresh.append(jnp.where(here, value, found[feature]))
                found = tuple(fresh)
            return found

        if owner == 0:
            found = (jnp.zeros((rows, LANES), jnp.float32),) * 4
        found = lax.fori_loop(0, table_rows // 2, one, found)
    lane = lax.broadcasted_iota(jnp.int32, (rows, LANES), 1)
    half = lax.broadcasted_iota(jnp.int32, (rows, LANES), 0) & 1
    valid = (half * LANES + lane) < counts[...]
    mass = jnp.where(valid, found[3] * (-SCALE * SCALE * SLOPE), 0.0)
    values = tuple(found[f] * SCALE for f in range(3)) + (mass,)
    for row in range(rows):
        for feature in range(4):
            at = (row % 2) * 4 + feature
            out[row // 2, at : at + 1, :] = values[feature][row : row + 1, :]


def pull_kernel(share, rows, counts, active_counts, pos, ranks, table, out, nodes, sinks, totals):
    visits = rows.shape[0] // active_counts.shape[0]
    block = pl.program_id(0)
    width = pos.shape[2]
    padded = sinks.shape[1]
    lane8 = lax.broadcasted_iota(jnp.int32, (8, LANES), 1)
    nodes[...] = jnp.zeros_like(nodes)

    def add_list(visit, offset):
        row = rows[block * visits + visit]
        safe = jnp.maximum(row, 0)
        entry = table[safe // share, pl.ds(pl.multiple_of(safe % share * 8, 8), 8), :]
        entry = jnp.where(row >= 0, entry, 0.0)
        shift = offset & (LANES - 1)
        base = (offset >> 7) * 4
        turned = pltpu.roll(entry, shift, 1)
        kept = lane8 >= shift
        nodes[pl.ds(base, 8), :] = jnp.where(kept, turned, nodes[pl.ds(base, 8), :])
        nodes[pl.ds(base + 4, 8), :] = jnp.where(kept, nodes[pl.ds(base + 4, 8), :], turned)
        return offset + jnp.where(row >= 0, counts[safe], 0)

    offset = jnp.int32(0)
    for visit in range(visits):
        offset = add_list(visit, offset)
    chunks = (offset + LANES - 1) >> 7
    steps = (active_counts[block] + STEP - 1) // STEP

    rank = ranks[0]
    order = lax.broadcasted_iota(jnp.int32, (padded, width), 0)
    chosen = order == jnp.broadcast_to(rank, (padded, width))
    whole = pos[0] * SCALE
    high = whole.astype(jnp.bfloat16)
    rest = whole - high.astype(jnp.float32)
    middle = rest.astype(jnp.bfloat16)
    last = (rest - middle.astype(jnp.float32)).astype(jnp.bfloat16)
    packed = jnp.where(chosen, 1.0, 0.0).astype(jnp.bfloat16)

    def pick(piece):
        return lax.dot_general(
            packed, piece, (((1,), (1,)), ((), ())), preferred_element_type=jnp.float32
        )

    picked = pick(high) + pick(middle) + pick(last)
    for axis in range(3):
        sinks[axis] = jnp.broadcast_to(picked[:, axis : axis + 1], (padded, LANES))
        totals[axis] = jnp.zeros((padded, LANES), jnp.float32)

    def one_chunk(chunk, carry):
        line = [
            jnp.broadcast_to(nodes[pl.ds(chunk * 4 + f, 1), :], (STEP, LANES)) for f in range(4)
        ]

        def one_step(step, carry):
            at = pl.ds(pl.multiple_of(step * STEP, 8), STEP)
            dx = sinks[0, at, :] - line[0]
            dy = sinks[1, at, :] - line[1]
            dz = sinks[2, at, :] - line[2]
            range_sq = dx * dx + dy * dy + (dz * dz + SOFTEN_SQ * SCALE * SCALE)
            inverse = lax.rsqrt(range_sq)
            distance = range_sq * inverse
            t = 1.0 / (distance + SHIFT)
            poly = t * POLY[-1] + POLY[-2]
            for coefficient in POLY[-3::-1]:
                poly = poly * t + coefficient
            factor = (t * poly + distance) * jnp.exp2(-range_sq)
            weight = (line[3] * inverse) * (inverse * inverse) * factor
            totals[0, at, :] += dx * weight
            totals[1, at, :] += dy * weight
            totals[2, at, :] += dz * weight
            return carry

        return lax.fori_loop(0, steps, one_step, carry)

    lax.fori_loop(0, chunks, one_chunk, 0)
    for axis in range(3):
        total = jnp.sum(totals[axis], axis=1, keepdims=True)
        spread = jnp.where(chosen, jnp.broadcast_to(total, (padded, width)), 0.0)
        out[0, axis : axis + 1, :] = jnp.sum(spread, axis=0, keepdims=True)


def local(
    positions,
    time_bins,
    home_groups,
    targets,
    target_groups,
    node_pos,
    node_mass,
    node_lists,
    list_counts,
):
    domains = lax.axis_size("dom")
    sharers = lax.axis_size("sub")
    domain = lax.axis_index("dom")
    place = lax.axis_index("sub")
    blocks, most_visits = targets.shape
    width = positions.shape[2]
    groups, length = node_lists.shape
    share = groups // sharers
    halves = length // LANES

    own = jnp.concatenate([node_pos, node_mass[None, :]], axis=0).reshape(4, -1, LANES)
    domain_nodes = lax.all_gather(own, "sub")

    ids = lax.dynamic_slice_in_dim(node_lists, place * share, share, 0).reshape(-1, LANES)
    own_counts = lax.dynamic_slice_in_dim(list_counts, place * share, share, 0)
    vmem = pl.BlockSpec(memory_space=pltpu.VMEM)
    tables = pl.pallas_call(
        gather_kernel,
        out_shape=jax.ShapeDtypeStruct((share, 8, LANES), jnp.float32),
        in_specs=[vmem] * 3,
        out_specs=vmem,
    )(domain_nodes, ids, jnp.repeat(own_counts, halves)[:, None])
    tail = jnp.zeros((8, LANES), jnp.float32)
    tail = tail.at[0, :share].set(own_counts.astype(jnp.float32))
    sent = jnp.concatenate([tables.reshape(share * 8, LANES), tail], axis=0)
    table = lax.all_gather(sent, ("dom", "sub"))
    counts = table[:, share * 8, :share].reshape(-1).astype(jnp.int32)

    is_active = time_bins <= CUR_BIN
    active_counts = jnp.sum(is_active.astype(jnp.int32), axis=1)
    lower = jnp.arange(width)[:, None] <= jnp.arange(width)[None, :]
    running = jnp.dot(
        is_active.astype(jnp.bfloat16),
        lower.astype(jnp.bfloat16),
        preferred_element_type=jnp.float32,
    ).astype(jnp.int32)
    ranks = jnp.where(is_active, running - 1, -1)[:, None, :]
    rows = jnp.concatenate(
        [
            (domain * groups + home_groups)[:, None],
            jnp.where(targets >= 0, targets * groups + target_groups, -1),
        ],
        axis=1,
    ).reshape(-1)

    visits = most_visits + 1
    padded = -(-width // STEP) * STEP
    grid_spec = pltpu.PrefetchScalarGridSpec(
        num_scalar_prefetch=3,
        grid=(blocks,),
        in_specs=[
            pl.BlockSpec((1, 3, width), lambda b, *_: (b, 0, 0)),
            pl.BlockSpec((1, 1, width), lambda b, *_: (b, 0, 0)),
            vmem,
        ],
        out_specs=pl.BlockSpec((1, 3, width), lambda b, *_: (b, 0, 0)),
        scratch_shapes=[
            pltpu.VMEM((-(-(visits * halves + 3) // 2) * 8, LANES), jnp.float32),
            pltpu.VMEM((3, padded, LANES), jnp.float32),
            pltpu.VMEM((3, padded, LANES), jnp.float32),
        ],
    )
    return pl.pallas_call(
        functools.partial(pull_kernel, share),
        out_shape=jax.ShapeDtypeStruct((blocks, 3, width), jnp.float32),
        grid_spec=grid_spec,
        compiler_params=pltpu.CompilerParams(vmem_limit_bytes=48 * 1024 * 1024),
    )(rows, counts, active_counts, positions, ranks, table)


def solution(mesh):
    return jax.shard_map(
        local,
        mesh=mesh,
        in_specs=(
            P(("dom", "sub"), None, None),
            P(("dom", "sub"), None),
            P(("dom", "sub")),
            P(("dom", "sub"), None),
            P(("dom", "sub"), None),
            P(None, ("dom", "sub")),
            P(("dom", "sub")),
            P("dom", None),
            P("dom"),
        ),
        out_specs=P(("dom", "sub"), None, None),
        check_vma=False,
    )
```

```python
import functools
import math

import jax
import jax.numpy as jnp
from jax import lax
from jax.experimental import pallas as pl
from jax.experimental.pallas import tpu as pltpu
from jax.sharding import PartitionSpec as P

CUR_BIN = 2
SOFTEN_SQ = 0.04
LANES = 128
SCALE = math.sqrt(math.log2(math.e) / 4)
SLOPE = 1.0 / (math.sqrt(math.pi) * SCALE)
SHIFT = 3.303086624162737
POLY = (
    0.7187441716120562,
    2.51274456019257,
    4.689033408702265,
    49.73417752543693,
    -125.5838890131009,
    722.0978767862518,
    -720.5249114117939,
)
MESH = pl.DeviceIdType.MESH
STEP = 72


def gather_kernel(nodes, ids, counts, out):
    sharers, _, table_rows, _ = nodes.shape
    rows = ids.shape[0]
    index = ids[...]
    high = index >> 7
    low = index & (LANES - 1)
    for owner in range(sharers):

        def one(step, found):
            for sub_step in range(2):
                row = step * 2 + sub_step
                here = high == owner * table_rows + row
                fresh = []
                for feature in range(4):
                    line = jnp.broadcast_to(nodes[owner, feature, pl.ds(row, 1), :], (rows, LANES))
                    value = jnp.take_along_axis(line, low, axis=1, mode="promise_in_bounds")
                    fresh.append(jnp.where(here, value, found[feature]))
                found = tuple(fresh)
            return found

        if owner == 0:
            found = (jnp.zeros((rows, LANES), jnp.float32),) * 4
        found = lax.fori_loop(0, table_rows // 2, one, found)
    lane = lax.broadcasted_iota(jnp.int32, (rows, LANES), 1)
    half = lax.broadcasted_iota(jnp.int32, (rows, LANES), 0) & 1
    valid = (half * LANES + lane) < counts[...]
    mass = jnp.where(valid, found[3] * (-SCALE * SCALE * SLOPE), 0.0)
    values = tuple(found[f] * SCALE for f in range(3)) + (mass,)
    for row in range(rows):
        for feature in range(4):
            at = (row % 2) * 4 + feature
            out[row // 2, at : at + 1, :] = values[feature][row : row + 1, :]


def share_nodes_kernel(own, out, send_sem, recv_sem):
    sharers = lax.axis_size("sub")
    place = lax.axis_index("sub")
    barrier = pltpu.get_barrier_semaphore()
    others = [lax.rem(place + k, sharers) for k in range(1, sharers)]
    for other in others:
        pl.semaphore_signal(barrier, inc=1, device_id={"sub": other}, device_id_type=MESH)
    pl.semaphore_wait(barrier, sharers - 1)
    copies = []
    for k, other in enumerate(others):
        copy = pltpu.make_async_remote_copy(
            src_ref=own,
            dst_ref=out.at[place],
            send_sem=send_sem.at[k],
            recv_sem=recv_sem.at[k],
            device_id={"sub": other},
            device_id_type=MESH,
        )
        copy.start()
        copies.append(copy)
    out[place] = own[...]
    for copy in copies:
        copy.wait()


def share_tables_kernel(own, out, send_sem, recv_sem, near_send, near_recv):
    half = lax.axis_size("sub") // 2
    chips = lax.axis_size("dom") * half
    domain, place = lax.axis_index("dom"), lax.axis_index("sub")
    core = lax.rem(place, 2)
    chip = domain * half + place // 2
    sibling = {"sub": place + 1 - 2 * core}

    def device(k):
        there = lax.rem(chip + k, chips)
        return {"dom": there // half, "sub": lax.rem(there, half) * 2 + core}

    def slot(k):
        return lax.rem(chip + chips - k, chips) * 2 + core

    barrier = pltpu.get_barrier_semaphore()
    pl.semaphore_signal(barrier, inc=1, device_id=sibling, device_id_type=MESH)

    @pl.loop(1, chips)
    def _(k):
        pl.semaphore_signal(barrier, inc=1, device_id=device(k), device_id_type=MESH)

    pl.semaphore_wait(barrier, chips)

    def far(k, at):
        return pltpu.make_async_remote_copy(
            src_ref=own,
            dst_ref=out.at[at],
            send_sem=send_sem.at[k],
            recv_sem=recv_sem.at[k],
            device_id=device(k),
            device_id_type=MESH,
        )

    def near(k, source):
        return pltpu.make_async_remote_copy(
            src_ref=source,
            dst_ref=out.at[slot(k)],
            send_sem=near_send.at[k],
            recv_sem=near_recv.at[k],
            device_id=sibling,
            device_id_type=MESH,
        )

    @pl.loop(1, chips)
    def _(k):
        far(k, slot(0)).start()

    near(0, own).start()
    out[slot(0)] = own[...]

    @pl.loop(1, chips)
    def _(k):
        far(k, slot(k)).wait_recv()
        near(k, out.at[slot(k)]).start()

    near(0, own).wait()

    @pl.loop(1, chips)
    def _(k):
        far(k, slot(0)).wait_send()
        near(k, out.at[slot(k)]).wait()


def pull_kernel(share, rows, counts, active_counts, pos, ranks, table, out, nodes, sinks, totals):
    visits = rows.shape[0] // active_counts.shape[0]
    block = pl.program_id(0)
    width = pos.shape[2]
    padded = sinks.shape[1]
    lane8 = lax.broadcasted_iota(jnp.int32, (8, LANES), 1)
    nodes[...] = jnp.zeros_like(nodes)

    def add_list(visit, offset):
        row = rows[block * visits + visit]
        safe = jnp.maximum(row, 0)
        entry = table[safe // share, pl.ds(pl.multiple_of(safe % share * 8, 8), 8), :]
        entry = jnp.where(row >= 0, entry, 0.0)
        shift = offset & (LANES - 1)
        base = (offset >> 7) * 4
        turned = pltpu.roll(entry, shift, 1)
        kept = lane8 >= shift
        nodes[pl.ds(base, 8), :] = jnp.where(kept, turned, nodes[pl.ds(base, 8), :])
        nodes[pl.ds(base + 4, 8), :] = jnp.where(kept, nodes[pl.ds(base + 4, 8), :], turned)
        return offset + jnp.where(row >= 0, counts[safe], 0)

    offset = jnp.int32(0)
    for visit in range(visits):
        offset = add_list(visit, offset)
    chunks = (offset + LANES - 1) >> 7
    steps = (active_counts[block] + STEP - 1) // STEP

    rank = ranks[0]
    order = lax.broadcasted_iota(jnp.int32, (padded, width), 0)
    chosen = order == jnp.broadcast_to(rank, (padded, width))
    whole = pos[0] * SCALE
    high = whole.astype(jnp.bfloat16)
    rest = whole - high.astype(jnp.float32)
    middle = rest.astype(jnp.bfloat16)
    last = (rest - middle.astype(jnp.float32)).astype(jnp.bfloat16)
    packed = jnp.where(chosen, 1.0, 0.0).astype(jnp.bfloat16)

    def pick(piece):
        return lax.dot_general(
            packed, piece, (((1,), (1,)), ((), ())), preferred_element_type=jnp.float32
        )

    picked = pick(high) + pick(middle) + pick(last)
    for axis in range(3):
        sinks[axis] = jnp.broadcast_to(picked[:, axis : axis + 1], (padded, LANES))
        totals[axis] = jnp.zeros((padded, LANES), jnp.float32)

    def one_chunk(chunk, carry):
        line = [
            jnp.broadcast_to(nodes[pl.ds(chunk * 4 + f, 1), :], (STEP, LANES)) for f in range(4)
        ]

        def one_step(step, carry):
            at = pl.ds(pl.multiple_of(step * STEP, 8), STEP)
            dx = sinks[0, at, :] - line[0]
            dy = sinks[1, at, :] - line[1]
            dz = sinks[2, at, :] - line[2]
            range_sq = dx * dx + dy * dy + (dz * dz + SOFTEN_SQ * SCALE * SCALE)
            inverse = lax.rsqrt(range_sq)
            distance = range_sq * inverse
            t = 1.0 / (distance + SHIFT)
            poly = t * POLY[-1] + POLY[-2]
            for coefficient in POLY[-3::-1]:
                poly = poly * t + coefficient
            factor = (t * poly + distance) * jnp.exp2(-range_sq)
            weight = (line[3] * inverse) * (inverse * inverse) * factor
            totals[0, at, :] += dx * weight
            totals[1, at, :] += dy * weight
            totals[2, at, :] += dz * weight
            return carry

        return lax.fori_loop(0, steps, one_step, carry)

    lax.fori_loop(0, chunks, one_chunk, 0)
    for axis in range(3):
        total = jnp.sum(totals[axis], axis=1, keepdims=True)
        spread = jnp.where(chosen, jnp.broadcast_to(total, (padded, width)), 0.0)
        out[0, axis : axis + 1, :] = jnp.sum(spread, axis=0, keepdims=True)


def local(
    positions,
    time_bins,
    home_groups,
    targets,
    target_groups,
    node_pos,
    node_mass,
    node_lists,
    list_counts,
):
    domains = lax.axis_size("dom")
    sharers = lax.axis_size("sub")
    domain = lax.axis_index("dom")
    place = lax.axis_index("sub")
    blocks, most_visits = targets.shape
    width = positions.shape[2]
    groups, length = node_lists.shape
    share = groups // sharers
    halves = length // LANES

    own = jnp.concatenate([node_pos, node_mass[None, :]], axis=0).reshape(4, -1, LANES)
    vmem = pl.BlockSpec(memory_space=pltpu.VMEM)
    dma = pltpu.SemaphoreType.DMA
    domain_nodes = pl.pallas_call(
        share_nodes_kernel,
        out_shape=jax.ShapeDtypeStruct((sharers,) + own.shape, jnp.float32),
        in_specs=[vmem],
        out_specs=vmem,
        scratch_shapes=[dma((sharers - 1,)), dma((sharers - 1,))],
        compiler_params=pltpu.CompilerParams(collective_id=0, has_side_effects=True),
    )(own)

    ids = lax.dynamic_slice_in_dim(node_lists, place * share, share, 0).reshape(-1, LANES)
    own_counts = lax.dynamic_slice_in_dim(list_counts, place * share, share, 0)
    tables = pl.pallas_call(
        gather_kernel,
        out_shape=jax.ShapeDtypeStruct((share, 8, LANES), jnp.float32),
        in_specs=[vmem] * 3,
        out_specs=vmem,
    )(domain_nodes, ids, jnp.repeat(own_counts, halves)[:, None])
    tail = jnp.zeros((8, LANES), jnp.float32)
    tail = tail.at[0, :share].set(own_counts.astype(jnp.float32))
    sent = jnp.concatenate([tables.reshape(share * 8, LANES), tail], axis=0)
    chips = domains * sharers // 2
    table = pl.pallas_call(
        share_tables_kernel,
        out_shape=jax.ShapeDtypeStruct((domains * sharers,) + sent.shape, jnp.float32),
        in_specs=[vmem],
        out_specs=vmem,
        scratch_shapes=[dma((chips,))] * 4,
        compiler_params=pltpu.CompilerParams(
            collective_id=1, has_side_effects=True, vmem_limit_bytes=48 * 1024 * 1024
        ),
    )(sent)
    counts = table[:, share * 8, :share].reshape(-1).astype(jnp.int32)

    is_active = time_bins <= CUR_BIN
    active_counts = jnp.sum(is_active.astype(jnp.int32), axis=1)
    lower = jnp.arange(width)[:, None] <= jnp.arange(width)[None, :]
    running = jnp.dot(
        is_active.astype(jnp.bfloat16),
        lower.astype(jnp.bfloat16),
        preferred_element_type=jnp.float32,
    ).astype(jnp.int32)
    ranks = jnp.where(is_active, running - 1, -1)[:, None, :]
    rows = jnp.concatenate(
        [
            (domain * groups + home_groups)[:, None],
            jnp.where(targets >= 0, targets * groups + target_groups, -1),
        ],
        axis=1,
    ).reshape(-1)

    visits = most_visits + 1
    padded = -(-width // STEP) * STEP
    grid_spec = pltpu.PrefetchScalarGridSpec(
        num_scalar_prefetch=3,
        grid=(blocks,),
        in_specs=[
            pl.BlockSpec((1, 3, width), lambda b, *_: (b, 0, 0)),
            pl.BlockSpec((1, 1, width), lambda b, *_: (b, 0, 0)),
            vmem,
        ],
        out_specs=pl.BlockSpec((1, 3, width), lambda b, *_: (b, 0, 0)),
        scratch_shapes=[
            pltpu.VMEM((-(-(visits * halves + 3) // 2) * 8, LANES), jnp.float32),
            pltpu.VMEM((3, padded, LANES), jnp.float32),
            pltpu.VMEM((3, padded, LANES), jnp.float32),
        ],
    )
    return pl.pallas_call(
        functools.partial(pull_kernel, share),
        out_shape=jax.ShapeDtypeStruct((blocks, 3, width), jnp.float32),
        grid_spec=grid_spec,
        compiler_params=pltpu.CompilerParams(vmem_limit_bytes=48 * 1024 * 1024),
    )(rows, counts, active_counts, positions, ranks, table)


def solution(mesh):
    return jax.shard_map(
        local,
        mesh=mesh,
        in_specs=(
            P(("dom", "sub"), None, None),
            P(("dom", "sub"), None),
            P(("dom", "sub")),
            P(("dom", "sub"), None),
            P(("dom", "sub"), None),
            P(None, ("dom", "sub")),
            P(("dom", "sub")),
            P("dom", None),
            P("dom"),
        ),
        out_specs=P(("dom", "sub"), None, None),
        check_vma=False,
    )
```
